32 devices in a mesh: rep: 1 (over z), r: 4 (over y), s: 8 (over x, core).
Axes of the slice: x: 4, y: 4, z: 1, core: 2. Of those that a mesh axis runs over, the one named last changes fastest.
The devices are a block of a 4x4x8 slice.
Arguments:
- x: bfloat16 [32, 2048, 1024], P(('rep', 'r', 's'))
- dy: bfloat16 [32, 2048, 1024], P(('rep', 'r', 's'))
- w_gate: bfloat16 [2, 1024, 3200], P(None, 's')
- w_up: bfloat16 [2, 1024, 3200], P(None, 's')
- w_down: bfloat16 [2, 3200, 1024], P(None, 's')
- m_w_gate: float32 [2, 1024, 3200], P(None, 's')
- m_w_up: float32 [2, 1024, 3200], P(None, 's')
- m_w_down: float32 [2, 3200, 1024], P(None, 's')
- v_w_gate: float32 [2, 1024, 3200], P(None, 's')
- v_w_up: float32 [2, 1024, 3200], P(None, 's')
- v_w_down: float32 [2, 3200, 1024], P(None, 's')
Outputs:
- output 1: bfloat16 [2, 1024, 3200], P('rep', 's')
- output 2: bfloat16 [2, 1024, 3200], P('rep', 's')
- output 3: bfloat16 [2, 3200, 1024], P('rep', 's')
- output 4: float32 [2, 1024, 3200], P('rep', 's')
- output 5: float32 [2, 1024, 3200], P('rep', 's')
- output 6: float32 [2, 3200, 1024], P('rep', 's')
- output 7: float32 [2, 1024, 3200], P('rep', 's')
- output 8: float32 [2, 1024, 3200], P('rep', 's')
- output 9: float32 [2, 3200, 1024], P('rep', 's')
All inputs are finite; a program needn't handle non-finite values.
Results may differ from the reference program's by a relative error of at most 0.022.
Values are sent between devices in bfloat16 or wider.
A program may use at most 768 MiB of HBM per device.

```python
import jax
import jax.numpy as jnp
from jax import lax

SEQUENCES = 32
TOKENS = 2048
D = 1024
FF = 3200
LAYERS = 2
NAMES = ("w_gate", "w_up", "w_down")
SHAPES = {"w_gate": (LAYERS, D, FF), "w_up": (LAYERS, D, FF), "w_down": (LAYERS, FF, D)}


def bump(key, n, height):
    away = (jnp.arange(n, dtype=jnp.int32) - jax.random.randint(key, (), 0, n, jnp.int32)) % n
    return jnp.where(away < n // 8, height, 1.0)


def together(key, own, strength):
    shared = jax.random.normal(key, own.shape[1:], jnp.float32)
    return (own + strength * shared) * lax.rsqrt(1 + strength * strength)


def setup_inputs(seed: int = 0, part: int = 0) -> dict:
    kx, kdy, ka, kb, kz, kf, kh, kl, *keys = jax.random.split(jax.random.key(seed), 8 + 3 * len(NAMES))
    kx, kdy, ka, kb = (jax.random.fold_in(k, part) for k in (kx, kdy, ka, kb))
    kw, km, kv = (keys[i::3] for i in range(3))
    shape = (SEQUENCES, TOKENS, D)
    much_x, much_dy = jax.random.uniform(kz, (2,), jnp.float32, 0.0, 1.0)
    loud = 2.0 ** jax.random.uniform(jax.random.fold_in(kz, 1), (), jnp.float32, -1.0, 2.0)
    layers = 2.0 ** jax.random.uniform(kl, (LAYERS, 1, 1), jnp.float32, -1.0, 1.0)
    x = together(ka, jax.random.normal(kx, shape, jnp.float32), much_x) * bump(kf, D, 4.0)
    dy = together(kb, jax.random.normal(kdy, shape, jnp.float32), much_dy)
    drawn = {"x": x.astype(jnp.bfloat16), "dy": (loud * dy * (SEQUENCES * TOKENS) ** -0.5).astype(jnp.bfloat16)}
    for key, name in zip(kw, NAMES, strict=True):
        w = jax.random.normal(key, SHAPES[name], jnp.float32) * SHAPES[name][1] ** -0.5
        drawn[name] = (w * {"w_gate": 1.0, "w_up": bump(kh, FF, 4.0), "w_down": layers}[name]).astype(jnp.bfloat16)
    for key, name in zip(km, NAMES, strict=True):
        drawn[f"m_{name}"] = 0.1 * jax.random.normal(key, SHAPES[name], jnp.float32)
    for key, name in zip(kv, NAMES, strict=True):
        drawn[f"v_{name}"] = jax.random.uniform(key, SHAPES[name], jnp.float32, 0.005, 0.015)
    return drawn


def matmul(a, w):
    return jnp.dot(a, w, preferred_element_type=jnp.float32).astype(jnp.bfloat16)


def normed(h):
    wide = h.astype(jnp.float32)
    scale = lax.rsqrt(jnp.mean(wide**2, -1, keepdims=True) + 1e-6)
    return (wide * scale).astype(jnp.bfloat16)


def layer(h, w):
    a = normed(h)
    gate = jnp.dot(a, w["w_gate"], preferred_element_type=jnp.float32)
    up = jnp.dot(a, w["w_up"], preferred_element_type=jnp.float32)
    return h + matmul((jax.nn.silu(gate) * up).astype(jnp.bfloat16), w["w_down"])


def adamw(w, m, v, g):
    m = 0.9 * m + 0.1 * g
    v = 0.95 * v + 0.05 * g * g
    step = m * lax.rsqrt(v + 1e-8) + 0.1 * w
    return (w - 0.02 * step).astype(jnp.bfloat16), m, v


def clipped(gradients, sum_of_squares, count):
    factor = jnp.minimum(1.0, 0.5 * lax.rsqrt(sum_of_squares / count + 1e-30))
    return [g * factor for g in gradients]


def stack(weights, h):
    return lax.scan(lambda h, w: (layer(h, w), None), h, weights)[0]


def reference(x, dy, w_gate, w_up, w_down, m_w_gate, m_w_up, m_w_down, v_w_gate, v_w_up, v_w_down):
    weights = dict(zip(NAMES, (w_gate, w_up, w_down), strict=True))

    def take(so_far, sequence):
        h, by_y = sequence
        _, back = jax.vjp(lambda w: stack(w, h), weights)
        return jax.tree.map(lambda total, term: total + term.astype(jnp.float32), so_far, back(by_y)[0]), None

    none_yet = {name: jnp.zeros(w.shape, jnp.float32) for name, w in weights.items()}
    by_weights, _ = lax.scan(take, none_yet, (x, dy))
    gradients = [by_weights[name].astype(jnp.bfloat16).astype(jnp.float32) for name in NAMES]
    gradients = clipped(gradients, sum(jnp.sum(g * g) for g in gradients), sum(g.size for g in gradients))
    new = [
        adamw(w.astype(jnp.float32), m, v, g)
        for w, m, v, g in zip((w_gate, w_up, w_down), (m_w_gate, m_w_up, m_w_down), (v_w_gate, v_w_up, v_w_down), gradients, strict=True)
    ]
    return tuple(one[which] for which in range(3) for one in new)
```

```python
import functools
import itertools

import jax
import jax.numpy as jnp
from jax import lax
from jax.experimental import pallas as pl
from jax.experimental.pallas import tpu as pltpu
from jax.sharding import PartitionSpec as P

MESH = pl.DeviceIdType.MESH
BF, F32 = jnp.bfloat16, jnp.float32
ANY = pl.BlockSpec(memory_space=pl.ANY)
NT, TN = (((1,), (1,)), ((), ())), (((0,), (0,)), ((), ()))
ROWS = 16


def dot(a, b, dims=None):
    if dims is None:
        return jnp.dot(a, b, preferred_element_type=F32)
    return lax.dot_general(a, b, dims, preferred_element_type=F32)


def like(shape, dtype=BF):
    return jax.ShapeDtypeStruct(shape, dtype)


def halves(rows):
    first = -(-rows // (2 * ROWS)) * ROWS
    return (0, first), (first, rows - first)


class Place:
    def __init__(self, ns, nr):
        s, y = lax.axis_index("s"), lax.axis_index("r")
        self.ns, self.nx, self.nr, self.s = ns, ns // 2, nr, s
        self.x, self.c, self.y = lax.div(s, 2), lax.rem(s, 2), y

    def block(self, offset, other=False):
        core = 1 - self.c if other else self.c
        return 2 * lax.rem(self.x + offset, self.nx) + core

    def to(self, name):
        if name == "partner":
            return {"s": self.block(0, True)}
        if name == "x+":
            return {"s": self.block(1)}
        if name == "x-":
            return {"s": self.block(self.nx - 1)}
        if name == "y+":
            return {"r": lax.rem(self.y + 1, self.nr)}
        if name == "y-":
            return {"r": lax.rem(self.y + self.nr - 1, self.nr)}
        return {"s": lax.rem(self.s + name, self.ns)}


def rows_of(block, rows, start=0, size=None):
    return pl.ds(pl.multiple_of(block * rows + start, ROWS), rows if size is None else size)


def add(out, terms, size, squares=None):
    rows, cols = size

    def window(where, i):
        ref, row, col = where
        return ref, (pl.ds(pl.multiple_of(i * ROWS + row, ROWS), ROWS), pl.ds(pl.multiple_of(col, 128), cols))

    def one(i, _):
        total = None
        for where in terms:
            ref, at = window(where, i)
            term = ref[at].astype(F32)
            total = term if total is None else total + term
        ref, at = window(out, i)
        ref[at] = total.astype(ref.dtype)
        return 0

    lax.fori_loop(0, rows // ROWS, one, 0)


class Comm:
    late = False

    def scratch(self):
        return self.buffers() + [
            pltpu.SemaphoreType.DMA((self.remote,)),
            pltpu.SemaphoreType.DMA((self.remote,)),
            pltpu.SemaphoreType.DMA((self.local,)),
        ]

    def bind(self, place, ins, outs, scratch):
        self.p, self.i, self.o = place, ins, outs
        self.b, (self.send, self.recv, self.here) = scratch[:-3], scratch[-3:]

    def far(self, k, src, dst, to):
        return pltpu.make_async_remote_copy(
            src_ref=src, dst_ref=dst, send_sem=self.send.at[k], recv_sem=self.recv.at[k],
            device_id=self.p.to(to), device_id_type=MESH,
        )

    def near(self, k, src, dst):
        return pltpu.make_async_copy(src, dst, self.here.at[k])


class Gather(Comm):
    remote, local = 9, 2
    peers = ("partner", "x+", "x-")

    def __init__(self, w, layer, ns):
        self.layer, self.ns = layer, ns
        self.rows, self.cols = w.shape[1:]
        self.ins, self.outs = [w], [like((ns * self.rows, self.cols))]

    def buffers(self):
        return [pltpu.VMEM((self.rows, self.cols), BF)]

    def copy(self, k):
        p, out, r = self.p, self.o[0], self.rows
        own = self.i[0].at[self.layer]
        if k < 3:
            return self.far(k, own, out.at[rows_of(p.block(0), r)], ("x+", "x-", "partner")[k])
        left, right, far = p.nx - 1, 1, 2
        offset = (left, right, left, right, far, far)[k - 3]
        part = None if k in (5, 6) else (k - 3) % 2
        start, size = (0, r) if part is None else halves(r)[part]
        where = out.at[rows_of(p.block(offset), r, start, size)]
        return self.far(k, where, where, self.peers[k - 2] if k < 5 else "partner")

    def start(self):
        for k in range(3):
            self.copy(k).start()
        self.near(0, self.i[0].at[self.layer], self.b[0]).start()

    def put(self):
        return self.near(1, self.b[0], self.o[0].at[rows_of(self.p.block(0), self.rows)])

    def e0(self):
        self.near(0, self.i[0].at[self.layer], self.b[0]).wait()
        self.put().start()
        self.copy(0).wait_recv()
        self.copy(3).start()
        self.copy(5).start()
        self.copy(1).wait_recv()
        self.copy(4).start()
        self.copy(6).start()

    def e1(self):
        for k in (3, 4):
            self.copy(k).wait_recv()
            self.copy(k + 4).start()

    def e2(self):
        for k in (2, *range(5, 9)):
            self.copy(k).wait_recv()
        for k in range(9):
            self.copy(k).wait_send()
        self.put().wait()

    def events(self):
        return [self.e0, self.e1, self.e2]


class GatherAcross(Comm):
    remote, local = 29, 2
    peers = ("partner", "x+", "x-", "y+", "y-")

    def __init__(self, w, layer, ns, nr):
        self.layer, self.part = layer, w.shape[1] // nr
        self.rows, self.cols = w.shape[1:]
        self.ins, self.outs = [w], [like((ns * self.rows, self.cols))]

    def buffers(self):
        return [pltpu.VMEM((self.rows, self.cols), BF)]

    def at(self, chip, group, half=None):
        p, q = self.p, self.part
        start = lax.rem(p.y + group, p.nr) * q
        size = q if half is None else q // 2
        return self.o[0].at[rows_of(p.block(chip), self.rows, start + (0 if half is None else half * size), size)]

    def copy(self, k):
        p, q = self.p, self.part
        own = self.i[0].at[self.layer]
        left, right, far = p.nx - 1, 1, 2
        if k == 0:
            return self.far(k, own, self.o[0].at[rows_of(p.block(0), self.rows)], "partner")
        if k < 3:
            return self.far(k, own.at[rows_of(p.y, q)], self.at(0, 0), ("x+", "x-")[k - 1])
        if k < 5:
            where = self.at((left, right)[k - 3], 0, k - 3)
            return self.far(k, where, where, ("x+", "x-")[k - 3])
        which, k1 = divmod(k - 5, 8)
        chip = (left, right, far)[which]
        if k1 < 2:
            where, to = self.at(chip, 0), ("y+", "y-")[k1]
        elif k1 < 4:
            where, to = self.at(chip, (p.nr - 1, 1)[k1 - 2], k1 - 2), ("y+", "y-")[k1 - 2]
        else:
            where, to = self.at(chip, (0, p.nr - 1, 1, 2)[k1 - 4]), "partner"
        return self.far(k, where, where, to)

    def start(self):
        for k in (1, 2, 0):
            self.copy(k).start()
        self.near(0, self.i[0].at[self.layer], self.b[0]).start()

    def put(self):
        return self.near(1, self.b[0], self.o[0].at[rows_of(self.p.block(0), self.rows)])

    def spread(self, which):
        for k in (0, 1, 4):
            self.copy(5 + 8 * which + k).start()

    def e0(self):
        self.near(0, self.i[0].at[self.layer], self.b[0]).wait()
        self.put().start()
        for which in range(2):
            self.copy(1 + which).wait_recv()
            self.copy(3 + which).start()
            self.spread(which)

    def e1(self):
        for k in (3, 4):
            self.copy(k).wait_recv()
        self.spread(2)

    def on(self, which):
        for k in range(2):
            self.copy(5 + 8 * which + k).wait_recv()
            self.copy(5 + 8 * which + 2 + k).start()
            self.copy(5 + 8 * which + 5 + k).start()

    def e2(self):
        self.on(0)
        self.on(1)

    def e3(self):
        self.on(2)

    def e4(self):
        for which in range(3):
            for k in (2, 3):
                self.copy(5 + 8 * which + k).wait_recv()
            self.copy(5 + 8 * which + 7).start()

    def e5(self):
        for k in [0] + [5 + 8 * which + j for which in range(3) for j in range(4, 8)]:
            self.copy(k).wait_recv()
        for k in range(29):
            self.copy(k).wait_send()
        self.put().wait()

    def events(self):
        return [self.e0, self.e1, self.e2, self.e3, self.e4, self.e5]


class Scatter(Comm):
    def __init__(self, g, ns, nr=None):
        self.rows, self.cols = g.shape[0] // ns, g.shape[1]
        self.pieces = 1 if nr is None else ns // 2
        self.ring = ("x+", "x-") if nr is None else ("y+", "y-")
        self.peers = ("partner",) + self.ring
        self.first = 4 * self.pieces
        self.remote, self.local = self.first + 6, self.first + 1
        self.ins, self.outs = [g], [like((self.rows, self.cols))]

    def buffers(self):
        r, c = self.rows, self.cols
        (_, a), (_, b) = halves(r)
        shapes = [(4, r, c), (4, r, c), (a, c), (b, c), (r, c), (r, c)]
        return [pltpu.VMEM(shape, BF) for shape in shapes]

    def source(self, j, piece, other):
        p, r = self.p, self.rows
        offset = (2, 1, 3, 0)[j]
        if self.pieces == 1:
            return self.i[0].at[rows_of(p.block(offset, other), r)]
        q = r // self.pieces
        core = 1 - p.c if other else p.c
        return self.i[0].at[rows_of(2 * piece + core, r, lax.rem(p.y + offset, p.nr) * q, q)]

    def into(self, ref, j, piece):
        q = self.rows // self.pieces
        return ref.at[j, pl.ds(piece * q, q)]

    def term(self, j, piece):
        return self.far(j * self.pieces + piece, self.source(j, piece, True), self.into(self.b[1], j, piece), "partner")

    def load(self, j, piece):
        return self.near(j * self.pieces + piece, self.source(j, piece, False), self.into(self.b[0], j, piece))

    def copy(self, k):
        own, ra, x1m, x1p, x2m, x2p = self.b
        (s0, n0), (s1, n1) = halves(self.rows)
        h0, h1 = pl.ds(s0, n0), pl.ds(s1, n1)
        src, dst, to = (
            (own.at[0, h0], x1m, 0),
            (own.at[0, h1], x1p, 1),
            (own.at[1, h1], x2m.at[h1], 0),
            (own.at[2, h0], x2p.at[h0], 1),
            (own.at[1, h0], x2m.at[h0], 0),
            (own.at[2, h1], x2p.at[h1], 1),
        )[k]
        return self.far(self.first + k, src, dst, self.ring[to])

    def start(self):
        for j in range(4):
            for piece in range(self.pieces):
                self.term(j, piece).start()
                self.load(j, piece).start()

    def ready(self, j):
        for piece in range(self.pieces):
            self.load(j, piece).wait()
            self.term(j, piece).wait_recv()

    def sum(self, j, half, *more):
        own, ra = self.b[0].at[j], self.b[1].at[j]
        start, size = (0, self.rows) if half is None else halves(self.rows)[half]
        add((own, start, 0), [(own, start, 0), (ra, start, 0)] + [(ref, 0, 0) for ref in more], (size, self.cols))

    def e0(self):
        self.ready(0)
        self.sum(0, 0)
        self.copy(0).start()
        self.sum(0, 1)
        self.copy(1).start()
        self.ready(1)
        self.sum(1, 1)
        self.copy(2).start()
        self.ready(2)
        self.sum(2, 0)
        self.copy(3).start()

    def e1(self):
        self.copy(0).wait_recv()
        self.sum(1, 0, self.b[2])
        self.copy(4).start()
        self.copy(1).wait_recv()
        self.sum(2, 1, self.b[3])
        self.copy(5).start()

    def e2(self):
        self.ready(3)
        for k in range(2, 6):
            self.copy(k).wait_recv()
        self.sum(3, None, self.b[4], self.b[5])
        put = self.near(self.first, self.b[0].at[3], self.o[0])
        put.start()
        for j in range(4):
            for piece in range(self.pieces):
                self.term(j, piece).wait_send()
        for k in range(6):
            self.copy(k).wait_send()
        put.wait()

    def events(self):
        return [self.e0, self.e1, self.e2]


class Finish(Comm):
    remote, local = 10, 3

    def __init__(self, block, along):
        self.rows, self.cols = block.shape
        self.by_rows = self.rows % (8 * ROWS) == 0
        self.along = along
        self.ring = (along + "+", along + "-")
        self.peers = self.ring + ("y+", "y-")
        self.ins, self.outs = [block], [like(block.shape), like((ROWS, 128), F32)]

    def buffers(self):
        full = (self.rows, self.cols)
        one = (self.rows // 4, self.cols) if self.by_rows else (self.rows, self.cols // 4)
        return [pltpu.VMEM(shape, BF) for shape in (full, full, self.window()[2], self.window()[2], one, one)] + [pltpu.VMEM((ROWS, 128), F32)]

    def window(self, fourth=0, half=0, halved=True):
        parts = 8 if halved else 4
        at = fourth * (parts // 4) + half
        if self.by_rows:
            return at * (self.rows // parts), 0, (self.rows // parts, self.cols)
        return 0, at * (self.cols // parts), (self.rows, self.cols // parts)

    def cut(self, ref, *which):
        row, col, (rows, cols) = self.window(*which)
        if self.by_rows:
            return ref.at[pl.ds(pl.multiple_of(row, ROWS), rows)]
        return ref.at[:, pl.ds(pl.multiple_of(col, 128), cols)]

    def near_by(self, offset):
        p = self.p
        return lax.rem(p.x + offset, p.nx) if self.along == "x" else lax.rem(p.y + offset, p.nr)

    def copy(self, k):
        p, block = self.p, self.i[0]
        own, res, r1m, r1p, r2m, r2p, _ = self.b
        plus, minus = self.ring
        if k < 6:
            src, dst, to = (
                (self.cut(block, self.near_by(2), 0), r1m, plus),
                (self.cut(block, self.near_by(2), 1), r1p, minus),
                (self.cut(block, self.near_by(1), 1), self.cut(r2m, 0, 1), plus),
                (self.cut(block, self.near_by(3), 0), self.cut(r2p, 0, 0), minus),
                (self.cut(own, self.near_by(1), 0), self.cut(r2m, 0, 0), plus),
                (self.cut(own, self.near_by(3), 1), self.cut(r2p, 0, 1), minus),
            )[k]
            return self.far(k, src, dst, to)
        if k < 8:
            where = self.cut(res, p.y, 0, False)
        else:
            where = self.cut(res, lax.rem(p.y + (p.nr - 1, 1)[k - 8], p.nr), k - 8)
        return self.far(k, where, where, ("y+", "y-")[k % 2])

    def start(self):
        for k in range(4):
            self.copy(k).start()
        self.near(0, self.i[0], self.b[0]).start()

    def e0(self):
        own, _, r1m, r1p = self.b[:4]
        self.near(0, self.i[0], own).wait()
        for k, (offset, half, ref) in enumerate(((1, 0, r1m), (3, 1, r1p))):
            self.copy(k).wait_recv()
            row, col, size = self.window(self.near_by(offset), half)
            add((own, row, col), [(own, row, col), (ref, 0, 0)], size)
            self.copy(4 + k).start()

    def e1(self):
        own, res, _, _, r2m, r2p, _ = self.b
        for k in range(2, 6):
            self.copy(k).wait_recv()
        row, col, size = self.window(self.near_by(0), 0, False)
        to_row, to_col, _ = self.window(self.p.y, 0, False)
        add((res, to_row, to_col), [(own, row, col), (r2m, 0, 0), (r2p, 0, 0)], size)
        self.copy(6).start()
        self.copy(7).start()

    def e2(self):
        for k in (6, 7):
            self.copy(k).wait_recv()
            self.copy(k + 2).start()

    def e3(self):
        res, squares = self.b[1], self.b[-1]
        self.copy(8).wait_recv()
        self.copy(9).wait_recv()
        self.near(1, res, self.o[0]).start()

        def one(i, total):
            g = res[pl.ds(pl.multiple_of(i * ROWS, ROWS), ROWS), :].astype(F32)
            g = g * g
            for j in range(self.cols // 128):
                total = total + g[:, 128 * j : 128 * (j + 1)]
            return total

        squares[...] = lax.fori_loop(0, self.rows // ROWS, one, jnp.zeros((ROWS, 128), F32))
        put = self.near(2, squares, self.o[1])
        put.start()
        for k in range(10):
            self.copy(k).wait_send()
        self.near(1, res, self.o[0]).wait()
        put.wait()

    def events(self):
        return [self.e0, self.e1, self.e2, self.e3]


class Total(Comm):
    def __init__(self, squares, last, ns):
        self.ns, self.last = ns, last
        self.remote, self.local = ns - 1, len(squares) + 1
        self.ins, self.outs = list(squares), [like((8, 128), F32)]
        self.peers = tuple(range(1, ns))

    def buffers(self):
        one = (ROWS, 128)
        return [pltpu.VMEM((len(self.ins),) + one, F32), pltpu.VMEM(one, F32), pltpu.VMEM((self.ns,) + one, F32), pltpu.VMEM((8, 128), F32)]

    def copy(self, k):
        return self.far(k - 1, self.b[1], self.b[2].at[self.p.s], k)

    def start(self):
        for j, ref in enumerate(self.i):
            self.near(j, ref, self.b[0].at[j]).start()

    def e0(self):
        loaded, mine, slots, out = self.b
        total = self.last[0].b[-1][...]
        for comm in self.last[1:]:
            total = total + comm.b[-1][...]
        for j, ref in enumerate(self.i):
            self.near(j, ref, loaded.at[j]).wait()
            total = total + loaded[j]
        mine[...] = total
        for k in range(1, self.ns):
            self.copy(k).start()
        slots[self.p.s] = total
        for k in range(1, self.ns):
            self.copy(k).wait_recv()
        total = slots[0]
        for k in range(1, self.ns):
            total = total + slots[k]
        out[...] = jnp.full((8, 128), jnp.sum(total), F32)
        put = self.near(len(self.i), out, self.o[0])
        put.start()
        for k in range(1, self.ns):
            self.copy(k).wait_send()
        put.wait()

    def events(self):
        return [self.e0]


def kernel(numbers, sizes, name, compute=None, steps=1, ins=(), outs=(), resident=(), comms=(), plan=(), due=None):
    order = []
    for which, (comm, steps_of) in enumerate(zip(comms, plan, strict=True)):
        events = comm.events()
        if len(steps_of) > len(events):
            events = [comm.start] + events
            comm.late = True
        order += [(at, max(j - comm.late, 0), which, event) for j, (at, event) in enumerate(zip(steps_of, events, strict=True))]
    order.sort(key=lambda entry: entry[:-1])
    ns, nr = sizes
    peers = tuple(dict.fromkeys(peer for comm in comms for peer in comm.peers))

    def body(*refs):
        refs = list(refs)

        def take(count):
            taken = refs[:count]
            del refs[:count]
            return taken

        my_ins, my_res = take(len(ins)), take(len(resident))
        comm_ins = [take(len(comm.ins)) for comm in comms]
        my_outs = take(len(outs))
        comm_outs = [take(len(comm.outs)) for comm in comms]
        held = take(len(resident))
        sems = take(1)[0] if resident else None
        place = Place(ns, nr)
        for comm, i, o in zip(comms, comm_ins, comm_outs, strict=True):
            comm.bind(place, i, o, take(len(comm.scratch())))
        i = pl.program_id(0)
        loads = [pltpu.make_async_copy(src, dst, sems.at[j]) for j, (src, dst) in enumerate(zip(my_res, held, strict=True))]

        @pl.when(i == 0)
        def _():
            for load in loads:
                load.start()
            if peers:
                barrier = pltpu.get_barrier_semaphore()
                for peer in peers:
                    pl.semaphore_signal(barrier, inc=1, device_id=place.to(peer), device_id_type=MESH)
                pl.semaphore_wait(barrier, len(peers))
            for comm in comms:
                if not comm.late:
                    comm.start()

        for load, step in zip(loads, due or [0] * len(loads), strict=True):
            pl.when(i == step)(load.wait)

        def run(now):
            for at, _, _, event in order:
                if now(at):
                    event()

        for step in sorted({at for at, *_ in order if at < steps}):
            pl.when(i == step)(lambda step=step: run(lambda at: at == step))
        if compute is not None:
            compute(i, held, my_ins, my_outs)
        if order:
            pl.when(i == steps - 1)(lambda: run(lambda at: at >= steps))

    scratch = [pltpu.VMEM(a.shape, a.dtype) for a in resident]
    if resident:
        scratch.append(pltpu.SemaphoreType.DMA((len(resident),)))
    for comm in comms:
        scratch += comm.scratch()
    results = pl.pallas_call(
        body,
        grid=(steps,),
        in_specs=[spec for _, spec in ins] + [ANY] * (len(resident) + sum(len(comm.ins) for comm in comms)),
        out_specs=[spec for _, spec in outs] + [ANY] * sum(len(comm.outs) for comm in comms),
        out_shape=[shape for shape, _ in outs] + [shape for comm in comms for shape in comm.outs],
        scratch_shapes=scratch,
        name=name,
        compiler_params=pltpu.CompilerParams(
            vmem_limit_bytes=62 << 20,
            dimension_semantics=("arbitrary",),
            **({"collective_id": next(numbers), "has_side_effects": True} if comms else {}),
        ),
    )(*[a for a, _ in ins], *resident, *[a for comm in comms for a in comm.ins])
    results = list(results)
    mine, rest = results[: len(outs)], results[len(outs) :]
    theirs = []
    for comm in comms:
        theirs.append(rest[: len(comm.outs)])
        rest = rest[len(comm.outs) :]
    return mine, theirs


def rows_spec(size, cols):
    return pl.BlockSpec((size, cols), lambda i: (i, 0))


def cols_spec(rows, size):
    return pl.BlockSpec((rows, size), lambda i: (0, i))


def whole(function):
    def compute(i, held, ins, outs):
        for out, value in zip(outs, function(*[ref[...] for ref in (*ins, *held)]), strict=True):
            out[...] = value

    return compute


def normed(wide):
    scale = lax.rsqrt(jnp.mean(wide * wide, -1, keepdims=True) + 1e-6)
    return (wide * scale).astype(BF), scale


def adamw(w, m, v, g):
    m = 0.9 * m + 0.1 * g
    v = 0.95 * v + 0.05 * g * g
    step = m * lax.rsqrt(v + 1e-8) + 0.1 * w
    return (w - 0.02 * step).astype(BF), m, v


def solution(mesh):
    sizes = ns, nr = mesh.shape["s"], mesh.shape["r"]

    def step(x, dy, *arrays):
        weights, m, v = (arrays[i : i + 3] for i in (0, 3, 6))
        w_gate, w_up, w_down = weights
        x, dy = x[0], dy[0]
        tokens, d = x.shape
        ff = w_gate.shape[2]
        tile = 256
        n = tokens // tile
        call = functools.partial(kernel, itertools.count(), sizes)
        thin, wide = rows_spec(tile, d), rows_spec(tile, ff)

        def matrices(layer):
            return [GatherAcross(w_gate, layer, ns, nr), GatherAcross(w_up, layer, ns, nr), Gather(w_down, layer, ns)]

        early, last = range(1, 7), (3, 4, 6, 7)
        _, ((wg0,), (wu0,), (wd0,)) = call("first", comms=matrices(0), plan=(early, early, (1, *range(4, 7))))

        @whole
        def forward(h, w_gate, w_up, w_down):
            a, _ = normed(h.astype(F32))
            gate, up = dot(a, w_gate), dot(a, w_up)
            sig = jax.nn.sigmoid(gate)
            silu = gate * sig
            act = (silu * up).astype(BF)
            h = h + dot(act, w_down).astype(BF)
            return a, up * slope(gate, sig), silu, act, h, normed(h.astype(F32))[0]

        def slope(gate, sig):
            return sig * (1.0 + gate * (1.0 - sig))

        narrow, broad, exact = (like((tokens, d)), thin), (like((tokens, ff)), wide), (like((tokens, ff), F32), wide)
        (a0, slope0, silu0, act0, h1, a1), ((wg1,), (wu1,), (wd1,)) = call(
            "forward", forward, n, [(x, thin)], [narrow, exact, exact, broad, narrow, narrow],
            (wg0, wu0, wd0), matrices(1), ((1, 2, 3, 5, 7, n), (1, 2, 4, 5, 7, n), (1, 5, 7, n)),
        )

        @whole
        def turn(a, dy, w_gate, w_up, w_down):
            dact = dot(dy, w_down, NT).astype(BF).astype(F32)
            gate, up = dot(a, w_gate), dot(a, w_up)
            sig = jax.nn.sigmoid(gate)
            silu = gate * sig
            return (silu * up).astype(BF), (dact * (up * slope(gate, sig))).astype(BF), (dact * silu).astype(BF)

        (act1, dgate1, dup1), _ = call("turn", turn, n, [(a1, thin), (dy, thin)], [broad] * 3, (wg1, wu1, wd1))

        @whole
        def product(act, dh):
            return (dot(act, dh, TN).astype(BF),)

        def by_down(act, dh, comms=(), plan=()):
            size = 5 * 128
            return call(
                "by_down", product, ff // size, [(act, cols_spec(tokens, size))],
                [(like((ff, d)), rows_spec(size, d))], (dh,), comms, plan,
            )

        def by_both(a, dgate, dup, comms, plan):
            size = 128
            k = d // size

            def products(i, held, ins, outs):
                for which, now in enumerate((i < k, i >= k)):
                    part = slice(which, which + 1)
                    pl.when(now)(lambda part=part: product(i, held[part], ins, outs[part]))

            return call(
                "by_both", products, 2 * k, [(a, pl.BlockSpec((tokens, size), lambda i: (0, lax.rem(i, k))))],
                [
                    (like((d, ff)), pl.BlockSpec((size, ff), lambda i: (jnp.minimum(i, k - 1), 0))),
                    (like((d, ff)), pl.BlockSpec((size, ff), lambda i: (jnp.maximum(i - k, 0), 0))),
                ],
                (dgate, dup), comms, plan, (0, k),
            )

        (gd1,), _ = by_down(act1, dy)
        (gg1, gu1), ((sd1,),) = by_both(a1, dgate1, dup1, [Scatter(gd1, ns)], [(2, 7, 14)])

        @whole
        def by_states(dgate, dup, h, dy, w_gate, w_up):
            da = (dot(dgate, w_gate, NT).astype(BF) + dot(dup, w_up, NT).astype(BF)).astype(F32)
            h = h.astype(F32)
            _, scale = normed(h)
            dh = da * scale - h * (scale * scale * scale * jnp.mean(da * h, -1, keepdims=True))
            return (dy + dh.astype(BF),)

        (dh1,), ((sg1,), (su1,)) = call(
            "by_states", by_states, n, [(dgate1, wide), (dup1, wide), (h1, thin), (dy, thin)], [narrow],
            (wg1, wu1), [Scatter(gg1, ns), Scatter(gu1, ns, nr)], [(1, 4, n)] * 2,
        )

        @whole
        def by_act(dh, slope, silu, w_down):
            dact = dot(dh, w_down, NT).astype(BF).astype(F32)
            return (dact * slope).astype(BF), (dact * silu).astype(BF)

        (dgate0, dup0), ((rd1, qd1),) = call(
            "by_act", by_act, n, [(dh1, thin), (slope0, wide), (silu0, wide)], [broad] * 2,
            (wd0,), [Finish(sd1, "y")], [last],
        )
        (gd0,), ((rg1, qg1),) = by_down(act0, dh1, [Finish(sg1, "y")], [(1, 2, 4, 5)])
        (gg0, gu0), ((sd0,), (ru1, qu1)) = by_both(a0, dgate0, dup0, [Scatter(gd0, ns), Finish(su1, "x")], [(3, 8, 15), (2, 4, 6, 9)])
        _, ((sg0,), (rd0, qd0), (su0,)) = call(
            "tail", comms=[Scatter(gg0, ns), Finish(sd0, "y"), Scatter(gu0, ns, nr)], plan=[(1, 4, 6), (2, 3, 3, 5), (2, 4, 6)]
        )
        finish = [Finish(sg0, "y"), Finish(su0, "x")]
        _, ((rg0, _), (ru0, _), (total,)) = call("last", comms=finish + [Total([qd1, qg1, qu1, qd0], finish, ns)], plan=[last, last, [n]])

        gradients = [jnp.stack(pair).astype(F32) for pair in ((rg0, rg1), (ru0, ru1), (rd0, rd1))]
        count = ns * sum(g.size for g in gradients)
        factor = jnp.minimum(1.0, 0.5 * lax.rsqrt(total[0, 0] / count + 1e-30))
        new = [adamw(w.astype(F32), m, v, g * factor) for w, m, v, g in zip(weights, m, v, gradients, strict=True)]
        return tuple(one[which] for which in range(len(weights)) for one in new)

    states, cut = P(("rep", "r", "s")), P(None, "s")
    return jax.shard_map(
        step,
        mesh=mesh,
        in_specs=(states, states) + (cut,) * 9,
        out_specs=(P("rep", "s"),) * 9,
        check_vma=False,
    )
```
